32 devices in a mesh: dp: 2 (over x), col: 4 (over z), row: 4 (over y, core).
Axes of the slice: x: 2, y: 2, z: 4, core: 2. Of those that a mesh axis runs over, the one named last changes fastest.
Arguments:
- pair_rep: bfloat16 [2048, 1024, 128], P(('dp', 'row'), 'col'), parts along dimension 0
- pair_mask: int32 [2048, 1024], P(('dp', 'row'), 'col'), parts along dimension 0
- norm_in: bfloat16 [128], replicated
- proj_left: bfloat16 [128, 128], replicated
- gate_left: bfloat16 [128, 128], replicated
- proj_right: bfloat16 [128, 128], replicated
- gate_right: bfloat16 [128, 128], replicated
- proj_gate: bfloat16 [128, 128], replicated
- norm_out: bfloat16 [128], replicated
- proj_out: bfloat16 [128, 128], replicated
Outputs:
- output: bfloat16 [2048, 1024, 128], P(('dp', 'row'), 'col'), parts along dimension 0
There are 2 independent parts. The reference program is written for one: setup_inputs(seed, part) draws one part's arguments, and reference() takes and returns one part's arrays. A program takes and returns all parts, laid end to end along the dimension named above; an argument that names none is the same for every part.
All inputs are finite; a program needn't handle non-finite values.
Results may differ from the reference program's by a relative error of at most 0.00617067.
Values are sent between devices in bfloat16 or wider.
A program may use at most 1 GiB of HBM per device.

```python
import jax
import jax.numpy as jnp
from jax import lax

SEQ = 1024
CZ = 128
CHAN = 128
ROW_BLOCK = SEQ // 8
LN_EPS = 1e-5


def layer_norm(values, gain_vec, red_axis):
    centre = values - jnp.mean(values, axis=red_axis, keepdims=True)
    spread = jnp.mean(centre * centre, axis=red_axis, keepdims=True)
    return centre * lax.rsqrt(spread + LN_EPS) * gain_vec


def normal_weight(rng_key, w_shape, std_scale):
    return (jax.random.normal(rng_key, w_shape, jnp.float32) * std_scale).astype(jnp.bfloat16)


def gain_vector(rng_key, gain_width):
    return (1.0 + 0.3 * jax.random.normal(rng_key, (gain_width,), jnp.float32)).astype(jnp.bfloat16)


def setup_inputs(seed: int = 0, part: int = 0) -> dict:
    part_key = jax.random.fold_in(jax.random.key(seed), part)
    pair_key, mask_key = jax.random.split(part_key)
    weight_keys = jax.random.split(jax.random.key(seed + 1), 8)
    pair_rep = jax.random.normal(pair_key, (SEQ, SEQ, CZ), jnp.float32).astype(jnp.bfloat16)
    residue_ok = (jax.random.randint(mask_key, (SEQ,), 0, 10) != 0).astype(jnp.int32)
    pair_mask = residue_ok[:, None] * residue_ok[None, :]
    return dict(
        pair_rep=pair_rep,
        pair_mask=pair_mask,
        norm_in=gain_vector(weight_keys[0], CZ),
        proj_left=normal_weight(weight_keys[1], (CZ, CHAN), CZ ** -0.5),
        gate_left=normal_weight(weight_keys[2], (CZ, CHAN), CZ ** -0.5),
        proj_right=normal_weight(weight_keys[3], (CZ, CHAN), CZ ** -0.5),
        gate_right=normal_weight(weight_keys[4], (CZ, CHAN), CZ ** -0.5),
        proj_gate=normal_weight(weight_keys[5], (CZ, CZ), CZ ** -0.5),
        norm_out=gain_vector(weight_keys[6], CHAN),
        proj_out=normal_weight(weight_keys[7], (CHAN, CZ), 2.0 * CHAN ** -0.5),
    )


def reference(pair_rep, pair_mask, norm_in, proj_left, gate_left, proj_right, gate_right, proj_gate, norm_out, proj_out):
    pair_f = pair_rep.astype(jnp.float32)
    normed = layer_norm(pair_f, norm_in.astype(jnp.float32), -1).astype(jnp.bfloat16)
    flat_x = normed.reshape(SEQ * SEQ, CZ)
    keep_f = pair_mask.astype(jnp.float32).reshape(SEQ * SEQ, 1)

    def gated_proj(w_value, w_gate):
        value_f = jnp.dot(flat_x, w_value, preferred_element_type=jnp.float32)
        gate_vals = jax.nn.sigmoid(jnp.dot(flat_x, w_gate, preferred_element_type=jnp.float32))
        return (keep_f * gate_vals * value_f).astype(jnp.bfloat16).T.reshape(CHAN, SEQ, SEQ)

    left_op = gated_proj(proj_left, gate_left)
    right_op = gated_proj(proj_right, gate_right)
    out_gate = jax.nn.sigmoid(jnp.dot(flat_x, proj_gate, preferred_element_type=jnp.float32))
    gate_blocks = out_gate.reshape(8, ROW_BLOCK, SEQ, CZ)
    left_blocks = left_op.reshape(CHAN, 8, ROW_BLOCK, SEQ).transpose(1, 0, 2, 3)
    pair_blocks = pair_f.reshape(8, ROW_BLOCK, SEQ, CZ)
    gain_out = norm_out.astype(jnp.float32)[:, None, None]

    def channel_product(operands):
        return jnp.dot(operands[0], operands[1].T, preferred_element_type=jnp.float32)

    def row_block(operands):
        left_blk, gate_blk, pair_blk = operands
        contracted = lax.map(channel_product, (left_blk, right_op))
        normed_o = layer_norm(contracted, gain_out, 0).astype(jnp.bfloat16)
        update = jnp.dot(normed_o.reshape(CHAN, ROW_BLOCK * SEQ).T, proj_out, preferred_element_type=jnp.float32)
        return (pair_blk + gate_blk * update.reshape(ROW_BLOCK, SEQ, CZ)).astype(jnp.bfloat16)

    new_pair = lax.map(row_block, (left_blocks, gate_blocks, pair_blocks))
    return new_pair.reshape(SEQ, SEQ, CZ)
```

```python
import functools

import jax
import jax.numpy as jnp
from jax import lax
from jax.experimental import pallas as pl
from jax.experimental.pallas import tpu as pltpu
from jax.sharding import PartitionSpec as P

LN_EPS = 1e-5
BF16 = jnp.bfloat16
F32 = jnp.float32
LANES = 128
ROWS = 16


def layer_norm(values, gain_vec, red_axis):
    centre = values - jnp.mean(values, axis=red_axis, keepdims=True)
    spread = jnp.mean(centre * centre, axis=red_axis, keepdims=True)
    return centre * lax.rsqrt(spread + LN_EPS) * gain_vec


def enter_body(pair_ref, mask_ref, gain_ref, ones_ref, spread_ref, normed_ref, own_ref):
    width = pair_ref.shape[-1]
    ones = ones_ref[...]
    keep = mask_ref[...].astype(BF16)

    def row_sum(values):
        return jnp.dot(values, ones, preferred_element_type=F32)

    for row in range(pair_ref.shape[0]):
        tile = pair_ref[row]
        centre = tile.astype(F32) - row_sum(tile) * (1.0 / width)
        square = centre * centre
        high = square.astype(BF16)
        low = (square - high.astype(F32)).astype(BF16)
        variance = (row_sum(high) + row_sum(low)) * (1.0 / width)
        normed = (centre * lax.rsqrt(variance + LN_EPS) * gain_ref[...]).astype(BF16)
        normed_ref[row] = normed
        kept = lax.dot_general(keep, spread_ref[row], (((0,), (0,)), ((), ())), preferred_element_type=F32)
        own_ref[row] = jnp.where(kept > 0.5, normed.astype(F32), 0.0).astype(BF16)


def enter(pair, mask, gain):
    block, width = 16, pair.shape[-1]
    tile_spec = pl.BlockSpec((block,) + pair.shape[1:], lambda i: (i, 0, 0))
    ones = jnp.ones((width, width), BF16)
    spread = jnp.broadcast_to(jnp.eye(block, dtype=BF16)[:, :, None], (block, block, width))
    return pl.pallas_call(
        enter_body,
        out_shape=[jax.ShapeDtypeStruct(pair.shape, BF16)] * 2,
        grid=(pair.shape[0] // block,),
        in_specs=[tile_spec, pl.BlockSpec((block, mask.shape[1]), lambda i: (i, 0)), pl.BlockSpec(gain.shape, lambda i: (0, 0)),
                  pl.BlockSpec(ones.shape, lambda i: (0, 0)), pl.BlockSpec(spread.shape, lambda i: (0, 0, 0))],
        out_specs=[tile_spec, tile_spec],
        name='enter',
    )(pair, mask, gain, ones, spread)


def project_body(starts, pick_ref, *refs):
    count = len(starts)
    tile_refs, (weight_ref, out_ref, turn_ref, held_ref, sems) = refs[:count], refs[count:]
    chan = out_ref.shape[0]
    here, last = pl.program_id(0), pl.num_programs(0)

    def fetch(block):
        for which in range(count):
            @pl.when(pick_ref[0] == which)
            def _():
                rows = pl.ds(starts[which] + block * ROWS, ROWS)
                slot = block % 2
                pltpu.make_async_copy(tile_refs[which].at[rows], held_ref.at[slot], sems.at[slot]).start()

    pl.when(here == 0)(lambda: fetch(here))
    pl.when(here + 1 < last)(lambda: fetch(here + 1))
    slot = here % 2
    pltpu.make_async_copy(tile_refs[0].at[pl.ds(0, ROWS)], held_ref.at[slot], sems.at[slot]).wait()
    for row in range(ROWS):
        both = lax.dot_general(weight_ref[...], held_ref[slot, row], (((1,), (1,)), ((), ())), preferred_element_type=F32)
        value = both[:chan] / (1.0 + jnp.exp(-both[chan:]))
        for half in range(turn_ref.shape[0]):
            turn_ref[half, pl.ds(row, chan, stride=ROWS), :] = value[:, half * LANES:(half + 1) * LANES]
    for half in range(turn_ref.shape[0]):
        out_ref[:, :, half * LANES:(half + 1) * LANES] = turn_ref[half].reshape(chan, ROWS, LANES).astype(BF16)


def project(tiles, starts, rows, pick, weight):
    _, cols, depth = tiles[0].shape
    chan = weight.shape[0] // 2
    return pl.pallas_call(
        functools.partial(project_body, tuple(starts)),
        out_shape=jax.ShapeDtypeStruct((chan, rows, cols), BF16),
        grid_spec=pltpu.PrefetchScalarGridSpec(
            num_scalar_prefetch=1,
            grid=(rows // ROWS,),
            in_specs=[pl.BlockSpec(memory_space=pl.ANY)] * len(tiles) + [pl.BlockSpec(weight.shape, lambda i, p: (0, 0))],
            out_specs=pl.BlockSpec((chan, ROWS, cols), lambda i, p: (0, i, 0)),
            scratch_shapes=[
                pltpu.VMEM((cols // LANES, chan * ROWS, LANES), F32),
                pltpu.VMEM((2, ROWS, cols, depth), BF16),
                pltpu.SemaphoreType.DMA((2,)),
            ],
        ),
        cost_estimate=pl.CostEstimate(flops=4 * rows * cols * depth * chan, bytes_accessed=4 * rows * cols * depth, transcendentals=rows * cols * chan),
        name='project',
    )(pick, *tiles, weight)


def joined(refs, chan):
    return refs[0][chan] if len(refs) == 1 else jnp.concatenate([ref[chan] for ref in refs], axis=0)


def contract_body(n_left, n_right, *refs):
    left_refs, right_refs = refs[:n_left], refs[n_left:n_left + n_right]
    prev_ref, out_ref = (refs[n_left + n_right] if len(refs) > n_left + n_right + 1 else None), refs[-1]
    halves, block = out_ref.shape[0], out_ref.shape[1]
    for chan in range(block):
        total = lax.dot_general(joined(left_refs, chan), joined(right_refs, chan), (((1,), (1,)), ((), ())), preferred_element_type=F32)
        for half in range(halves):
            piece = total[:, half * LANES:(half + 1) * LANES]
            out_ref[half, chan] = piece if prev_ref is None else piece + prev_ref[half, chan]


def contract(lefts, rights, prev=None, first_half=0):
    chan, _, depth = lefts[0].shape
    rows, cols = sum(a.shape[1] for a in lefts), sum(a.shape[1] for a in rights)
    halves, block = cols // LANES, 8
    args = list(lefts) + list(rights)
    specs = [pl.BlockSpec((block,) + a.shape[1:], lambda c: (c, 0, 0)) for a in args]
    if prev is not None:
        args.append(prev)
        specs.append(pl.BlockSpec((halves, block, rows, LANES), lambda c: (first_half // halves, c, 0, 0)))
    return pl.pallas_call(
        functools.partial(contract_body, len(lefts), len(rights)),
        out_shape=jax.ShapeDtypeStruct((halves, chan, rows, LANES), F32),
        grid=(chan // block,),
        in_specs=specs,
        out_specs=pl.BlockSpec((halves, block, rows, LANES), lambda c: (0, c, 0, 0)),
        cost_estimate=pl.CostEstimate(flops=2 * chan * rows * cols * depth, bytes_accessed=4 * chan * rows * (depth + cols), transcendentals=0),
        name='contract',
    )(*args)


def finish_body(sum_ref, pair_ref, normed_ref, gain_ref, proj_ref, gate_ref, *rest):
    out_ref = rest[-1]
    _, chan, rows, _ = sum_ref.shape
    for row in range(rows):
        value = sum_ref.at[0].reshape(chan * rows, LANES)[pl.ds(row, chan, stride=rows), :]
        normed_o = layer_norm(value, gain_ref[...], 0).astype(BF16)
        update = lax.dot_general(normed_o, proj_ref[...], (((0,), (0,)), ((), ())), preferred_element_type=F32)
        gate = jnp.dot(normed_ref[row], gate_ref[...], preferred_element_type=F32)
        out_ref[row] = (pair_ref[row].astype(F32) + update / (1.0 + jnp.exp(-gate))).astype(BF16)


def finish(total, pair, normed, gain, proj_out, proj_gate, half, so_far=None):
    _, chan, rows, _ = total.shape
    block = 16
    gain = jnp.broadcast_to(gain[:, None], (chan, LANES))
    tile_spec = pl.BlockSpec((block, LANES, pair.shape[2]), lambda i: (i, half, 0))
    args = [total, pair, normed, gain, proj_out, proj_gate]
    specs = [pl.BlockSpec((1, chan, block, LANES), lambda i: (0, 0, i, 0)), tile_spec, tile_spec]
    specs += [pl.BlockSpec(a.shape, lambda i: (0, 0)) for a in args[3:]]
    if so_far is not None:
        args.append(so_far)
        specs.append(pl.BlockSpec(memory_space=pl.ANY))
    return pl.pallas_call(
        finish_body,
        out_shape=jax.ShapeDtypeStruct(pair.shape, BF16),
        grid=(rows // block,),
        in_specs=specs,
        out_specs=tile_spec,
        input_output_aliases={} if so_far is None else {6: 0},
        cost_estimate=pl.CostEstimate(flops=2 * pair.size * chan, bytes_accessed=5 * pair.size, transcendentals=pair.size // 2),
        name='finish',
    )(*args)


def solution(mesh):
    tile_spec = P(('dp', 'row'), 'col', None)
    mask_spec = P(('dp', 'row'), 'col')
    n = mesh.shape['row']
    both = ('col', 'row')
    swap_ends = [(0, 1), (1, 0), (2, 3), (3, 2)]
    swap_mids = [(1, 2), (2, 1)]
    to_ends = [(1, 0), (2, 3)]
    every, mids, ends = (0, 1, 2, 3), (1, 2), (0, 3)
    parts_last = 4

    def across(cols):
        return [(c * n + c, c * n + (c + 2) % n) for c in cols]

    def beside(cols):
        return [(c * n + c, c * n + (c ^ 1)) for c in cols]

    def beside_far(cols):
        return [(c * n + (c + 2) % n, c * n + ((c + 2) % n ^ 1)) for c in cols]

    def tile_program(pair, mask, norm_in, proj_left, gate_left, proj_right, gate_right, proj_gate, norm_out, proj_out):
        col, row = lax.axis_index('col'), lax.axis_index('row')
        at_end = jnp.where((col == 0) | (col == 3), 1, 0)
        role = jnp.where(row == col, 0, jnp.where(row == (col + 2) % n, 1, jnp.where(row // 2 == col // 2, 2, 3)))
        w_left = jnp.concatenate([proj_left.T, gate_left.T], axis=0)
        w_right = jnp.concatenate([proj_right.T, gate_right.T], axis=0)
        rows = pair.shape[0]
        step = rows // parts_last
        normed, own = enter(pair, mask, norm_in.astype(F32)[None, :])

        def pick(value):
            return jnp.asarray(value, jnp.int32).reshape(1)

        pick_own, pick_end, pick_role, pick_both = pick(0), pick(at_end), pick(role), pick(role + 4 * at_end)

        def move(tile, axes, pairs):
            return lax.ppermute(tile, axes, pairs)

        def spread(tile, cols):
            far = move(tile, both, across(cols))
            by = move(tile, both, beside(cols))
            return [tile, far, by, move(far, both, beside_far(cols))]

        def whole(tiles, which, weight):
            return project(tiles, [0] * len(tiles), rows, which, weight)

        near = move(own, 'col', swap_ends)
        mid2 = move(own, 'col', swap_mids)
        mid3 = move(near, 'col', swap_mids)
        end2 = move(mid2, 'col', to_ends)
        end3 = [move(lax.slice_in_dim(mid3, p * step, (p + 1) * step, axis=0), 'col', to_ends) for p in range(parts_last)]
        y_0, y_1 = spread(own, every), spread(near, every)
        y_2 = spread(mid2, mids) + spread(end2, ends)
        y_3m = spread(mid3, mids)
        y_3e = [spread(tile, ends) for tile in end3]

        total = contract([whole([own], pick_own, w_left)], [whole(y_0, pick_role, w_right)])
        total = contract([whole([near], pick_own, w_left)], [whole(y_1, pick_role, w_right)], total)
        total = contract([whole([mid2, end2], pick_end, w_left)], [whole(y_2, pick_both, w_right)], total)
        left = [project([mid3, end3[p]], [p * step, 0], step, pick_end, w_left) for p in range(parts_last)]
        right = [project(y_3m + y_3e[p], [p * step] * 4 + [0] * 4, step, pick_both, w_right) for p in range(parts_last)]
        out = None
        per_half = parts_last // 2
        for half in range(2):
            part = contract(left, right[half * per_half:(half + 1) * per_half], total, half)
            out = finish(part, pair, normed, norm_out.astype(F32), proj_out, proj_gate, half, out)
        return out

    return jax.shard_map(tile_program, mesh=mesh, in_specs=(tile_spec, mask_spec) + (P(),) * 8, out_specs=tile_spec, check_vma=False)
```
